256 devices in a mesh: seq: 4 (over x), batch: 64 (over z, y, core).
Axes of the slice: x: 4, y: 4, z: 8, core: 2. Of those that a mesh axis runs over, the one named last changes fastest.
Arguments:
- activations: bfloat16 [64, 3072, 4096], P('batch', 'seq'), may hold values from -48 to 48
- out_grads: bfloat16 [64, 3072, 4096], P('batch', 'seq'), may hold values from -0.875 to 0.875
- lengths: int32 [64, 3], P('batch'), may hold values from 1 to 1536, 3072 in all within a row
Outputs:
- act_factor: float32 [4096, 4096], P(('seq', 'batch'))
- grad_factor: float32 [4096, 4096], P(('seq', 'batch'))
The draws below stay inside these ranges and needn't reach their ends.
Inputs may be any that keep to these rules, and one draw needn't show every extreme that they name: `lengths`: each row sums to 3072 and its largest entry is exactly 1536.
All inputs are finite; a program needn't handle non-finite values.
Results may differ from the reference program's by a relative error of at most 0.004.
Values may be sent and summed in bfloat16 or wider, within the bound.
A program may use at most 64 MiB of HBM per device.

```python
import math
import jax
import jax.numpy as jnp
import numpy as np
from jax import lax

D = 4096
SEQS = 3
GROUP_TOK = 3072
MOST = 1536
GROUPS = 64
TOTAL_SEQS = 192


def with_spikes(values, stream_key, source, target, shards_of, factor):
    def block_of(dim):
        return (jnp.arange(values.shape[dim]) // (values.shape[dim] // shards_of)).reshape((-1,) + (1,) * (values.ndim - 1 - dim))

    one_side = jax.random.permutation(stream_key, shards_of)[block_of(target)]
    far = (block_of(target) + shards_of // 2) % shards_of
    return jnp.where((block_of(source) == one_side) | (block_of(source) == far), factor * values, values)


def shard_levels(own_key, extent, shards, least, high):
    def one(dim, shards_of):
        heights = jax.random.uniform(jax.random.fold_in(jax.random.fold_in(own_key, 6), dim), (shards_of,), jnp.float32, least / len(shards), high / len(shards))
        return jnp.repeat(jnp.exp(heights), extent[dim] // shards_of).reshape((-1,) + (1,) * (len(extent) - dim - 1))

    gain = one(*shards[0])
    for cut in shards[1:]:
        gain = gain * one(*cut)
    return gain


def split_up(count, total, reach, skew):
    weights = [(1 << 20) // math.isqrt(grade ** skew) + 1 for grade in range(2, count + 1)]
    rest, given = total - reach - (count - 1), [1] * (count - 1)
    while rest > 0:
        free = [i for i in range(count - 1) if given[i] < reach]
        mass, remaining = sum([weights[i] for i in free]), rest
        for i in free:
            more = min(reach - given[i], max(1, remaining * weights[i] // mass), rest)
            given[i] = given[i] + more
            rest = rest - more
    return np.array([reach] + given)


def uneven(key, number_of, total, reach, skew):
    if number_of == 2:
        one = jax.random.randint(key, (), max(1, total - reach), min(reach, total - 1) + 1)
        return jnp.stack([one, total - one])
    sizes = jnp.asarray(split_up(number_of, total, reach, skew), jnp.int32)
    twos = (number_of - 1) // 2
    source_of, taker = sizes[1:1 + 2 * twos:2], sizes[2:2 + 2 * twos:2]
    margin = jnp.minimum(source_of - 1, reach - taker)
    shifted = jax.random.randint(jax.random.fold_in(key, 1), (twos,), 0, 1 << 20) % (margin + 1)
    sizes = sizes.at[1:1 + 2 * twos:2].set(source_of - shifted).at[2:2 + 2 * twos:2].set(taker + shifted)
    return sizes[jax.random.permutation(jax.random.fold_in(key, 2), number_of)]


def bell_draw_with(stream_key, shape, width, most, split, heavy, held_as=jnp.bfloat16):
    array = width * jax.random.normal(stream_key, shape, jnp.float32)
    if split:
        array = array * shard_levels(stream_key, shape, split, -0.22, 0.18)
    return jnp.clip(with_spikes(array, jax.random.fold_in(stream_key, 3), *heavy), -most, most).astype(held_as)


def setup_inputs(seed: int = 0) -> dict:
    seeds = jax.random.split(jax.random.key(seed), 4)
    activations = bell_draw_with(seeds[0], (GROUPS, GROUP_TOK, D), 3.0, 48.0, ((0, 64), (1, 4)), (0, 2, 64, 4.0))
    out_grads = bell_draw_with(seeds[1], (GROUPS, GROUP_TOK, D), 0.05, 0.875, ((0, 64), (1, 4)), (0, 2, 64, 4.0))
    lengths = jax.vmap(lambda own: uneven(own, SEQS, GROUP_TOK, MOST, 2))(jax.random.split(seeds[2], GROUPS)).reshape((GROUPS, SEQS)).astype(jnp.int32)
    return dict(activations=activations, out_grads=out_grads, lengths=lengths)


def reference(activations, out_grads, lengths):
    ends = jnp.cumsum(lengths, axis=1).astype(jnp.int32)
    starts = ends - lengths
    position = jnp.arange(GROUP_TOK, dtype=jnp.int32)

    def reduce_group(item):
        act_group, grad_group, first, last = item
        member = (position[None, :] >= first[:, None]) & (position[None, :] < last[:, None])
        member = member.astype(jnp.bfloat16)
        act_sum = jnp.dot(member, act_group, preferred_element_type=jnp.float32)
        grad_sum = jnp.dot(member, grad_group, preferred_element_type=jnp.float32)
        return act_sum, grad_sum

    act_sum, grad_sum = lax.map(reduce_group, (activations, out_grads, starts, ends))
    act_rows = (act_sum / lengths[:, :, None].astype(jnp.float32)).astype(jnp.bfloat16).reshape(TOTAL_SEQS, D)
    grad_rows = grad_sum.astype(jnp.bfloat16).reshape(TOTAL_SEQS, D)
    act_factor = jnp.dot(act_rows.T, act_rows, preferred_element_type=jnp.float32) / TOTAL_SEQS
    grad_factor = jnp.dot(grad_rows.T, grad_rows, preferred_element_type=jnp.float32) / TOTAL_SEQS
    return act_factor, grad_factor
```

```python
import jax
import jax.numpy as jnp
from jax import lax
from jax.experimental import pallas as pl
from jax.experimental.pallas import tpu as pltpu
from jax.sharding import PartitionSpec as P

NX, NY, NZ, NC = 4, 4, 8, 2
NB = NY * NC
LANES = 128
SEQS = 3
MESH = pl.DeviceIdType.MESH
F32, BF16 = jnp.float32, jnp.bfloat16


def kernel(
    act_hbm, grad_hbm, len_ref, out_ref,
    abuf, gbuf, parts, got, packed, rhs, lhs, tiles, landed,
    in_sem, s1_send, s1_recv, z_send, z_recv, x_send, x_recv, l_send, l_recv, o_send, o_recv,
):
    steps, tokens, wide = abuf.shape
    halves = steps // NX
    per_step = wide // LANES
    total_seqs = SEQS * NZ * NY * NC
    rows = LANES // NB
    chunk = 2 * SEQS * NB

    x = lax.axis_index("seq")
    b = lax.axis_index("batch")
    c = b % NC
    y = (b // NC) % NY
    z = b // (NC * NY)
    mine = y + NY * c
    g_me = y * NC + c

    def at(x_, y_, z_, c_):
        return (x_, (z_ * NY + y_) * NC + c_)

    def quarter(i):
        return (x + 1 + i // halves) % NX

    def loads(i):
        cols = pl.ds(pl.multiple_of(quarter(i) * (halves * wide) + (i % halves) * wide, wide), wide)
        return (
            pltpu.make_async_copy(act_hbm.at[0, :, cols], abuf.at[i], in_sem.at[0, i]),
            pltpu.make_async_copy(grad_hbm.at[0, :, cols], gbuf.at[i], in_sem.at[1, i]),
        )

    @pl.loop(0, steps)
    def _(i):
        for copy in loads(i):
            copy.start()

    barrier = pltpu.get_barrier_semaphore()

    def greet(target):
        pl.semaphore_signal(barrier, inc=1, device_id=target, device_id_type=MESH)

    @pl.loop(1, NX * NB)
    def _(k):
        other = (x * NB + g_me + k) % (NX * NB)
        greet(at(other // NB, (other % NB) // NC, z, other % NC))

    @pl.loop(1, NZ)
    def _(k):
        greet(at(x, y, (z + k) % NZ, c))

    src_y, src_c = z % NY, z // NY
    src_here = jnp.logical_and(src_y == y, src_c == c)

    @pl.loop(0, NZ)
    def _(k):
        @pl.when(jnp.logical_not(jnp.logical_and(src_here, k == z)))
        def _():
            greet(at(x, src_y, k, src_c))

    l0, l1, l2 = len_ref[0, 0], len_ref[0, 1], len_ref[0, 2]
    row = lax.broadcasted_iota(jnp.int32, (8, tokens), 0)
    pos = lax.broadcasted_iota(jnp.int32, (8, tokens), 1) + x * tokens

    def member(first):
        r = row - first
        start = jnp.where(r == 0, 0, jnp.where(r == 1, l0, l0 + l1))
        end = jnp.where(r == 0, l0, jnp.where(r == 1, l0 + l1, l0 + l1 + l2))
        inside = (r >= 0) & (r < SEQS) & (pos >= start) & (pos < end)
        return jnp.where(inside, 1.0, 0.0).astype(BF16)

    m_act, m_grad = member(0), member(SEQS)
    row_w = lax.broadcasted_iota(jnp.int32, (8, wide), 0)
    divisor = jnp.where(row_w == 0, l0, jnp.where(row_w == 1, l1, jnp.where(row_w == 2, l2, 1))).astype(F32)

    def s1_copy(slot_block, target, slot):
        return pltpu.make_async_remote_copy(
            src_ref=parts.at[slot_block], dst_ref=got.at[slot],
            send_sem=s1_send, recv_sem=s1_recv, device_id=target, device_id_type=MESH,
        )

    my_slot = x * NB + g_me
    home = x * NB + mine

    @pl.loop(0, steps)
    def _(i):
        for copy in loads(i):
            copy.wait()
        total = jnp.dot(m_act, abuf[i], preferred_element_type=F32)
        total += jnp.dot(m_grad, gbuf[i], preferred_element_type=F32)
        total = total / divisor
        q = quarter(i)
        first = q * NB + (i % halves) * per_step
        for j in range(per_step):
            parts[first + j] = total[:, j * LANES : (j + 1) * LANES]

        @pl.when(i == 0)
        def _():
            pl.semaphore_wait(barrier, NX * NB - 1 + NZ - 1 + NZ - jnp.where(mine == z, 1, 0))

        for j in range(per_step):
            zb = (i % halves) * per_step + j

            @pl.when(first + j != home)
            def _():
                s1_copy(first + j, at(q, zb % NY, z, zb // NY), my_slot).start()

    got[my_slot] = parts[home]
    pltpu.make_async_copy(got.at[pl.ds(0, NX * NB - 1)], got.at[pl.ds(0, NX * NB - 1)], s1_recv).wait()

    for g in range(NB):
        summed = got[g]
        for k in range(1, NX):
            summed += got[k * NB + g]
        packed[g * SEQS : (g + 1) * SEQS] = summed[0:SEQS]
        packed[SEQS * (NB + g) : SEQS * (NB + g + 1)] = summed[SEQS : 2 * SEQS]
    own = packed[...].astype(BF16)
    rhs[x, z] = own

    @pl.when(mine == z)
    def _():
        lhs[z] = own

    def z_copy(k):
        return pltpu.make_async_remote_copy(
            src_ref=rhs.at[x, z], dst_ref=rhs.at[x, z],
            send_sem=z_send, recv_sem=z_recv.at[z],
            device_id=at(x, y, (z + k) % NZ, c), device_id_type=MESH,
        )

    def x_copy(k, layer):
        return pltpu.make_async_remote_copy(
            src_ref=rhs.at[x, layer], dst_ref=rhs.at[x, layer],
            send_sem=x_send, recv_sem=x_recv.at[x],
            device_id=at((x + k) % NX, y, z, c), device_id_type=MESH,
        )

    def l_copy(d):
        return pltpu.make_async_remote_copy(
            src_ref=rhs.at[x, z], dst_ref=lhs.at[z],
            send_sem=l_send, recv_sem=l_recv.at[z],
            device_id=at(x, d // NC, mine, d % NC), device_id_type=MESH,
        )

    for k in (4, 3, 5, 2, 6, 1, 7):
        z_copy(k).start()
    for k in (2, 1, 3):
        x_copy(k, z).start()
    for k in range(NB):
        d = (g_me + 4 + k) % NB

        @pl.when(jnp.logical_not(jnp.logical_and(mine == z, d == g_me)))
        def _():
            l_copy(d).start()

    def arrived(ref, sem):
        pltpu.make_async_copy(ref, ref, sem).wait()

    for k in (1, 7, 2, 6, 3, 5, 4):
        layer = (z + k) % NZ
        arrived(rhs.at[x, layer], z_recv.at[layer])
        for kx in (2, 1, 3):
            x_copy(kx, layer).start()

    for k in range(NZ):
        @pl.when(jnp.logical_not(jnp.logical_and(src_here, k == z)))
        def _():
            arrived(lhs.at[k], l_recv.at[k])

    depth = NZ * chunk
    lcols = lhs[...].reshape(depth, LANES)
    in_act = lax.broadcasted_iota(jnp.int32, (depth, LANES), 0) % chunk < SEQS * NB
    act_only = jnp.where(in_act, 1.0, 0.0).astype(BF16)
    grad_only = jnp.where(in_act, 0.0, 1.0).astype(BF16)
    both = jnp.concatenate([lcols * act_only, lcols * grad_only], axis=1)

    for k in range(1, NX):
        who = (x + k) % NX
        arrived(rhs.at[who], x_recv.at[who])

    for k in range(NX):
        product = lax.dot_general(
            both, rhs[k].reshape(depth, LANES), (((0,), (0,)), ((), ())), preferred_element_type=F32
        )
        product = (product / total_seqs).astype(BF16)
        for d in range(NB):
            for kind in range(2):
                tiles[d, kind * rows : (kind + 1) * rows, k * LANES : (k + 1) * LANES] = product[
                    kind * LANES + d * rows : kind * LANES + (d + 1) * rows
                ]

    def o_copy(d):
        return pltpu.make_async_remote_copy(
            src_ref=tiles.at[d], dst_ref=landed.at[mine],
            send_sem=o_send, recv_sem=o_recv,
            device_id=at(x, d // NC, z, d % NC), device_id_type=MESH,
        )

    for k in (4, 5, 2, 3, 6, 7, 1):
        d = (g_me + k) % NB
        o_copy(d).start()
    landed[mine] = tiles[g_me]

    arrived(got.at[pl.ds(0, NX * NB - 1)], s1_send)
    arrived(rhs.at[0, pl.ds(0, NZ - 1)], z_send)
    arrived(rhs.at[pl.ds(0, NX - 1)], x_send)

    @pl.when(mine == z)
    def _():
        arrived(lhs.at[pl.ds(0, NB - 1)], l_send)

    @pl.when(mine != z)
    def _():
        arrived(lhs.at[pl.ds(0, NB)], l_send)

    arrived(landed.at[pl.ds(0, NB - 1)], o_recv)
    arrived(landed.at[pl.ds(0, NB - 1)], o_send)
    for q in range(NX):
        for zb in range(NB):
            cols = pl.ds((q * NB + zb) * LANES, LANES)
            for kind in range(2):
                out_ref[kind, :, cols] = landed[zb, kind * rows : (kind + 1) * rows, q * LANES : (q + 1) * LANES]


def local(activations, out_grads, lengths):
    tokens, width = activations.shape[1:]
    rows = width // (NX * NY * NZ * NC)
    steps = 2 * NX
    wide = width // steps
    chunk = 2 * SEQS * NB
    dma = pltpu.SemaphoreType.DMA
    out = pl.pallas_call(
        kernel,
        out_shape=jax.ShapeDtypeStruct((2, rows, width), BF16),
        in_specs=[
            pl.BlockSpec(memory_space=pl.ANY),
            pl.BlockSpec(memory_space=pl.ANY),
            pl.BlockSpec(memory_space=pltpu.SMEM),
        ],
        out_specs=pl.BlockSpec(memory_space=pltpu.VMEM),
        scratch_shapes=[
            pltpu.VMEM((steps, tokens, wide), BF16),
            pltpu.VMEM((steps, tokens, wide), BF16),
            pltpu.VMEM((NX * NB, 8, LANES), F32),
            pltpu.VMEM((NX * NB, 8, LANES), F32),
            pltpu.VMEM((chunk, LANES), F32),
            pltpu.VMEM((NX, NZ, chunk, LANES), BF16),
            pltpu.VMEM((NZ, chunk, LANES), BF16),
            pltpu.VMEM((NB, 2 * rows, NX * LANES), BF16),
            pltpu.VMEM((NB, 2 * rows, NX * LANES), BF16),
            dma((2, steps)),
            dma, dma,
            dma, dma((NZ,)),
            dma, dma((NX,)),
            dma, dma((NZ,)),
            dma, dma,
        ],
        compiler_params=pltpu.CompilerParams(collective_id=0, has_side_effects=True),
    )(activations, out_grads, lengths)
    wide_out = out.astype(F32)
    return wide_out[0], wide_out[1]


def solution(mesh):
    in_specs = (P("batch", "seq", None), P("batch", "seq", None), P("batch", None))
    out_specs = (P(("seq", "batch"), None), P(("seq", "batch"), None))
    return jax.shard_map(local, mesh=mesh, in_specs=in_specs, out_specs=out_specs, check_vma=False)
```

```python
import jax
import jax.numpy as jnp
from jax import lax
from jax.experimental import pallas as pl
from jax.experimental.pallas import tpu as pltpu
from jax.sharding import PartitionSpec as P

NX, NY, NZ, NC = 4, 4, 8, 2
NB = NY * NC
LANES = 128
SEQS = 3
MESH = pl.DeviceIdType.MESH
F32, BF16 = jnp.float32, jnp.bfloat16


def kernel(
    act_hbm, grad_hbm, len_ref, out_ref,
    abuf, gbuf, parts, got, packed, rhs, lhs, tiles, landed,
    in_sem, s1_send, s1_recv, z_send, z_recv, x_send, x_recv, l_send, l_recv, o_send, o_recv,
):
    steps, tokens, wide = abuf.shape
    halves = steps // NX
    per_step = wide // LANES
    total_seqs = SEQS * NZ * NY * NC
    rows = LANES // NB
    chunk = 2 * SEQS * NB

    x = lax.axis_index("seq")
    b = lax.axis_index("batch")
    c = b % NC
    y = (b // NC) % NY
    z = b // (NC * NY)
    mine = y + NY * c
    g_me = y * NC + c

    def at(x_, y_, z_, c_):
        return (x_, (z_ * NY + y_) * NC + c_)

    def quarter(i):
        return (x + 1 + i // halves) % NX

    def loads(i):
        cols = pl.ds(pl.multiple_of(quarter(i) * (halves * wide) + (i % halves) * wide, wide), wide)
        return (
            pltpu.make_async_copy(act_hbm.at[0, :, cols], abuf.at[i], in_sem.at[0, i]),
            pltpu.make_async_copy(grad_hbm.at[0, :, cols], gbuf.at[i], in_sem.at[1, i]),
        )

    @pl.loop(0, steps)
    def _(i):
        for copy in loads(i):
            copy.start()

    barrier = pltpu.get_barrier_semaphore()

    def greet(target):
        pl.semaphore_signal(barrier, inc=1, device_id=target, device_id_type=MESH)

    @pl.loop(1, NX * NB)
    def _(k):
        other = (x * NB + g_me + k) % (NX * NB)
        greet(at(other // NB, (other % NB) // NC, z, other % NC))

    @pl.loop(1, NZ)
    def _(k):
        greet(at(x, y, (z + k) % NZ, c))

    src_y, src_c = z % NY, z // NY
    src_here = jnp.logical_and(src_y == y, src_c == c)

    @pl.loop(0, NZ)
    def _(k):
        @pl.when(jnp.logical_not(jnp.logical_and(src_here, k == z)))
        def _():
            greet(at(x, src_y, k, src_c))

    l0, l1, l2 = len_ref[0, 0], len_ref[0, 1], len_ref[0, 2]
    row = lax.broadcasted_iota(jnp.int32, (8, tokens), 0)
    pos = lax.broadcasted_iota(jnp.int32, (8, tokens), 1) + x * tokens

    def member(first):
        r = row - first
        start = jnp.where(r == 0, 0, jnp.where(r == 1, l0, l0 + l1))
        end = jnp.where(r == 0, l0, jnp.where(r == 1, l0 + l1, l0 + l1 + l2))
        inside = (r >= 0) & (r < SEQS) & (pos >= start) & (pos < end)
        return jnp.where(inside, 1.0, 0.0).astype(BF16)

    m_act, m_grad = member(0), member(SEQS)
    row_w = lax.broadcasted_iota(jnp.int32, (8, wide), 0)
    divisor = jnp.where(row_w == 0, l0, jnp.where(row_w == 1, l1, jnp.where(row_w == 2, l2, 1))).astype(F32)

    def s1_copy(slot_block, target, slot):
        return pltpu.make_async_remote_copy(
            src_ref=parts.at[slot_block], dst_ref=got.at[slot],
            send_sem=s1_send, recv_sem=s1_recv, device_id=target, device_id_type=MESH,
        )

    my_slot = x * NB + g_me
    home = x * NB + mine

    def sums(i):
        for copy in loads(i):
            copy.wait()
        total = jnp.dot(m_act, abuf[i], preferred_element_type=F32)
        total += jnp.dot(m_grad, gbuf[i], preferred_element_type=F32)
        total = total / divisor
        q = quarter(i)
        first = q * NB + (i % halves) * per_step
        for j in range(per_step):
            parts[first + j] = total[:, j * LANES : (j + 1) * LANES]

    def sends(i):
        q = quarter(i)
        first = q * NB + (i % halves) * per_step
        for j in range(per_step):
            zb = (i % halves) * per_step + j

            @pl.when(first + j != home)
            def _():
                s1_copy(first + j, at(q, zb % NY, z, zb // NY), my_slot).start()

    @pl.loop(0, 4)
    def _(i):
        sums(i)

    pl.semaphore_wait(barrier, NX * NB - 1 + NZ - 1 + NZ - jnp.where(mine == z, 1, 0))

    @pl.loop(0, 4)
    def _(i):
        sends(i)

    @pl.loop(4, steps)
    def _(i):
        sums(i)
        sends(i)

    got[my_slot] = parts[home]
    pltpu.make_async_copy(got.at[pl.ds(0, NX * NB - 1)], got.at[pl.ds(0, NX * NB - 1)], s1_recv).wait()

    for g in range(NB):
        summed = got[g]
        for k in range(1, NX):
            summed += got[k * NB + g]
        packed[g * SEQS : (g + 1) * SEQS] = summed[0:SEQS]
        packed[SEQS * (NB + g) : SEQS * (NB + g + 1)] = summed[SEQS : 2 * SEQS]
    own = packed[...].astype(BF16)
    rhs[x, z] = own

    @pl.when(mine == z)
    def _():
        lhs[z] = own

    def z_copy(k):
        return pltpu.make_async_remote_copy(
            src_ref=rhs.at[x, z], dst_ref=rhs.at[x, z],
            send_sem=z_send, recv_sem=z_recv.at[z],
            device_id=at(x, y, (z + k) % NZ, c), device_id_type=MESH,
        )

    def x_copy(k, layer):
        return pltpu.make_async_remote_copy(
            src_ref=rhs.at[x, layer], dst_ref=rhs.at[x, layer],
            send_sem=x_send, recv_sem=x_recv.at[x],
            device_id=at((x + k) % NX, y, z, c), device_id_type=MESH,
        )

    def l_copy(d):
        return pltpu.make_async_remote_copy(
            src_ref=rhs.at[x, z], dst_ref=lhs.at[z],
            send_sem=l_send, recv_sem=l_recv.at[z],
            device_id=at(x, d // NC, mine, d % NC), device_id_type=MESH,
        )

    for k in (4, 3, 5, 2, 6, 1, 7):
        z_copy(k).start()
    for k in (2, 1, 3):
        x_copy(k, z).start()
    for k in range(NB):
        d = (g_me + 4 + k) % NB

        @pl.when(jnp.logical_not(jnp.logical_and(mine == z, d == g_me)))
        def _():
            l_copy(d).start()

    def arrived(ref, sem):
        pltpu.make_async_copy(ref, ref, sem).wait()

    for k in (1, 7, 2, 6, 3, 5, 4):
        layer = (z + k) % NZ
        arrived(rhs.at[x, layer], z_recv.at[layer])
        for kx in (2, 1, 3):
            x_copy(kx, layer).start()

    for k in range(NZ):
        @pl.when(jnp.logical_not(jnp.logical_and(src_here, k == z)))
        def _():
            arrived(lhs.at[k], l_recv.at[k])

    depth = NZ * chunk
    lcols = lhs[...].reshape(depth, LANES)
    in_act = lax.broadcasted_iota(jnp.int32, (depth, LANES), 0) % chunk < SEQS * NB
    act_only = jnp.where(in_act, 1.0, 0.0).astype(BF16)
    grad_only = jnp.where(in_act, 0.0, 1.0).astype(BF16)
    both = jnp.concatenate([lcols * act_only, lcols * grad_only], axis=1)

    for k in (0, 1, 3, 2):
        who = (x + k) % NX
        if k:
            arrived(rhs.at[who], x_recv.at[who])
        product = lax.dot_general(
            both, rhs[who].reshape(depth, LANES), (((0,), (0,)), ((), ())), preferred_element_type=F32
        )
        product = (product / total_seqs).astype(BF16)
        for d in range(NB):
            for kind in range(2):
                tiles[k, d, kind * rows : (kind + 1) * rows] = product[
                    kind * LANES + d * rows : kind * LANES + (d + 1) * rows
                ]
        for step in (4, 5, 2, 3, 6, 7, 1):
            d = (g_me + step) % NB
            pltpu.make_async_remote_copy(
                src_ref=tiles.at[k, d], dst_ref=landed.at[who, mine],
                send_sem=o_send.at[k], recv_sem=o_recv.at[who],
                device_id=at(x, d // NC, z, d % NC), device_id_type=MESH,
            ).start()
        landed[who, mine] = tiles[k, g_me]

    arrived(got.at[pl.ds(0, NX * NB - 1)], s1_send)
    arrived(rhs.at[0, pl.ds(0, NZ - 1)], z_send)
    arrived(rhs.at[pl.ds(0, NX - 1)], x_send)

    @pl.when(mine == z)
    def _():
        arrived(lhs.at[pl.ds(0, NB - 1)], l_send)

    @pl.when(mine != z)
    def _():
        arrived(lhs.at[pl.ds(0, NB)], l_send)

    for k in range(NX):
        arrived(landed.at[k, pl.ds(0, NB - 1)], o_send.at[k])
    for q in range(NX):
        arrived(landed.at[q, pl.ds(0, NB - 1)], o_recv.at[q])
    for q in range(NX):
        for zb in range(NB):
            cols = pl.ds((q * NB + zb) * LANES, LANES)
            for kind in range(2):
                out_ref[kind, :, cols] = landed[q, zb, kind * rows : (kind + 1) * rows]


def local(activations, out_grads, lengths):
    tokens, width = activations.shape[1:]
    rows = width // (NX * NY * NZ * NC)
    steps = 2 * NX
    wide = width // steps
    chunk = 2 * SEQS * NB
    dma = pltpu.SemaphoreType.DMA
    out = pl.pallas_call(
        kernel,
        out_shape=pltpu.VMEM((2, rows, width), BF16),
        in_specs=[
            pl.BlockSpec(memory_space=pl.ANY),
            pl.BlockSpec(memory_space=pl.ANY),
            pl.BlockSpec(memory_space=pltpu.SMEM),
        ],
        out_specs=pl.BlockSpec(memory_space=pltpu.VMEM),
        scratch_shapes=[
            pltpu.VMEM((steps, tokens, wide), BF16),
            pltpu.VMEM((steps, tokens, wide), BF16),
            pltpu.VMEM((NX * NB, 8, LANES), F32),
            pltpu.VMEM((NX * NB, 8, LANES), F32),
            pltpu.VMEM((chunk, LANES), F32),
            pltpu.VMEM((NX, NZ, chunk, LANES), BF16),
            pltpu.VMEM((NZ, chunk, LANES), BF16),
            pltpu.VMEM((NX, NB, 2 * rows, LANES), BF16),
            pltpu.VMEM((NX, NB, 2 * rows, LANES), BF16),
            dma((2, steps)),
            dma, dma,
            dma, dma((NZ,)),
            dma, dma((NX,)),
            dma, dma((NZ,)),
            dma((NX,)), dma((NX,)),
        ],
        compiler_params=pltpu.CompilerParams(collective_id=0, has_side_effects=True),
    )(activations, out_grads, lengths)
    return out[0].astype(F32), out[1].astype(F32)


def solution(mesh):
    in_specs = (P("batch", "seq", None), P("batch", "seq", None), P("batch", None))
    out_specs = (P(("seq", "batch"), None), P(("seq", "batch"), None))
    return jax.shard_map(local, mesh=mesh, in_specs=in_specs, out_specs=out_specs, check_vma=False)
```

```python
import jax
import jax.numpy as jnp
from jax import lax
from jax.experimental import pallas as pl
from jax.experimental.pallas import tpu as pltpu
from jax.sharding import PartitionSpec as P

NX, NY, NZ, NC = 4, 4, 8, 2
NB = NY * NC
LANES = 128
SEQS = 3
HELD = 4
MESH = pl.DeviceIdType.MESH
F32, BF16 = jnp.float32, jnp.bfloat16


def kernel(
    act_hbm, grad_hbm, len_ref, out_ref,
    abuf, gbuf, parts, got, packed, rhs, lhs, tiles, landed,
    in_sem, s1_send, s1_recv, z_send, z_recv, x_send, x_recv, l_send, l_recv, d_send, o_send, o_recv,
):
    steps, tokens, wide = abuf.shape
    halves = steps // NX
    per_step = wide // LANES
    total_seqs = SEQS * NZ * NY * NC
    rows = LANES // NB
    chunk = 2 * SEQS * NB

    x = lax.axis_index("seq")
    b = lax.axis_index("batch")
    c = b % NC
    y = (b // NC) % NY
    z = b // (NC * NY)
    mine = y + NY * c
    g_me = y * NC + c

    def at(x_, y_, z_, c_):
        return (x_, (z_ * NY + y_) * NC + c_)

    def quarter(i):
        return (x + 1 + i // halves) % NX

    def loads(i):
        cols = pl.ds(pl.multiple_of(quarter(i) * (halves * wide) + (i % halves) * wide, wide), wide)
        return (
            pltpu.make_async_copy(act_hbm.at[0, :, cols], abuf.at[i], in_sem.at[0, i]),
            pltpu.make_async_copy(grad_hbm.at[0, :, cols], gbuf.at[i], in_sem.at[1, i]),
        )

    @pl.loop(0, steps)
    def _(i):
        for copy in loads(i):
            copy.start()

    barrier = pltpu.get_barrier_semaphore()

    def greet(target):
        pl.semaphore_signal(barrier, inc=1, device_id=target, device_id_type=MESH)

    src_y, src_c = z % NY, z // NY
    src_here = jnp.logical_and(src_y == y, src_c == c)

    for k in (4, 3, 5, 2, 6, 1, 7, 0):
        layer = (z + k) % NZ

        if k:
            greet(at(x, y, layer, c))

        @pl.when((layer % NC == c) & jnp.logical_not(src_here & (layer == z)))
        def _():
            greet(at(x, src_y, layer, src_c))

    for dx in (2, 1, 3, 0):
        for dy in (2, 1, 3, 0):
            for dc in range(NC):
                if dx or dy or dc:
                    greet(at((x + dx) % NX, (y + dy) % NY, z, (c + dc) % NC))

    l0, l1, l2 = len_ref[0, 0], len_ref[0, 1], len_ref[0, 2]
    row = lax.broadcasted_iota(jnp.int32, (8, tokens), 0)
    pos = lax.broadcasted_iota(jnp.int32, (8, tokens), 1) + x * tokens

    def member(first):
        r = row - first
        start = jnp.where(r == 0, 0, jnp.where(r == 1, l0, l0 + l1))
        end = jnp.where(r == 0, l0, jnp.where(r == 1, l0 + l1, l0 + l1 + l2))
        inside = (r >= 0) & (r < SEQS) & (pos >= start) & (pos < end)
        return jnp.where(inside, 1.0, 0.0).astype(BF16)

    m_act, m_grad = member(0), member(SEQS)
    row_w = lax.broadcasted_iota(jnp.int32, (8, wide), 0)
    divisor = jnp.where(row_w == 0, l0, jnp.where(row_w == 1, l1, jnp.where(row_w == 2, l2, 1))).astype(F32)

    def s1_copy(slot_block, target, slot):
        return pltpu.make_async_remote_copy(
            src_ref=parts.at[slot_block], dst_ref=got.at[slot],
            send_sem=s1_send, recv_sem=s1_recv, device_id=target, device_id_type=MESH,
        )

    my_slot = x * NB + g_me
    home = x * NB + mine

    def sums(i):
        for copy in loads(i):
            copy.wait()
        total = jnp.dot(m_act, abuf[i], preferred_element_type=F32)
        total += jnp.dot(m_grad, gbuf[i], preferred_element_type=F32)
        total = total / divisor
        q = quarter(i)
        first = q * NB + (i % halves) * per_step
        for j in range(per_step):
            parts[first + j] = total[:, j * LANES : (j + 1) * LANES]

    def sends(i):
        q = quarter(i)
        first = q * NB + (i % halves) * per_step
        for j in range(per_step):
            zb = (i % halves) * per_step + j

            @pl.when(first + j != home)
            def _():
                s1_copy(first + j, at(q, zb % NY, z, zb // NY), my_slot).start()

    for i in range(HELD):
        sums(i)

    pl.semaphore_wait(barrier, NX * NB - 1 + NZ - 1 + NY - jnp.where((mine == z) & (z % NC == c), 1, 0))

    @pl.loop(0, HELD)
    def _(i):
        sends(i)

    for i in range(HELD, steps):
        sums(i)
        sends(i)

    got[my_slot] = parts[home]
    pltpu.make_async_copy(got.at[pl.ds(0, NX * NB - 1)], got.at[pl.ds(0, NX * NB - 1)], s1_recv).wait()

    for g in range(NB):
        summed = got[g]
        for k in range(1, NX):
            summed += got[k * NB + g]
        packed[g * SEQS : (g + 1) * SEQS] = summed[0:SEQS]
        packed[SEQS * (NB + g) : SEQS * (NB + g + 1)] = summed[SEQS : 2 * SEQS]
    own = packed[...].astype(BF16)
    rhs[x, z] = own

    @pl.when((mine == z) & (z % NC == c))
    def _():
        lhs[z] = own

    def z_copy(k):
        return pltpu.make_async_remote_copy(
            src_ref=rhs.at[x, z], dst_ref=rhs.at[x, z],
            send_sem=z_send, recv_sem=z_recv.at[z],
            device_id=at(x, y, (z + k) % NZ, c), device_id_type=MESH,
        )

    def x_copy(k, layer):
        return pltpu.make_async_remote_copy(
            src_ref=rhs.at[x, layer], dst_ref=rhs.at[x, layer],
            send_sem=x_send, recv_sem=x_recv.at[x],
            device_id=at((x + k) % NX, y, z, c), device_id_type=MESH,
        )

    def l_copy(d):
        return pltpu.make_async_remote_copy(
            src_ref=rhs.at[x, z], dst_ref=lhs.at[z],
            send_sem=l_send, recv_sem=l_recv.at[z],
            device_id=at(x, d // NC, mine, d % NC), device_id_type=MESH,
        )

    for k in (4, 3, 5, 2, 6, 1, 7):
        z_copy(k).start()
    for k in (2, 1, 3):
        x_copy(k, z).start()
    for k in (2, 1, 3, 0):
        to_y = (y + k) % NY

        @pl.when(jnp.logical_not((mine == z) & (z % NC == c) & (to_y == y)))
        def _():
            l_copy(to_y * NC + z % NC).start()

    def arrived(ref, sem):
        pltpu.make_async_copy(ref, ref, sem).wait()

    for k in (1, 7, 2, 6, 3, 5, 4):
        layer = (z + k) % NZ
        arrived(rhs.at[x, layer], z_recv.at[layer])
        for kx in (2, 1, 3):
            x_copy(kx, layer).start()

    def hand_over(layer):
        return pltpu.make_async_remote_copy(
            src_ref=lhs.at[layer], dst_ref=lhs.at[layer],
            send_sem=d_send, recv_sem=l_recv.at[layer],
            device_id=at(x, y, z, 1 - c), device_id_type=MESH,
        )

    for k in range(NZ // NC):
        layer = (z + c + z % NC + (0, 6, 2, 4)[k]) % NZ

        @pl.when(jnp.logical_not(src_here & (layer == z)))
        def _():
            arrived(lhs.at[layer], l_recv.at[layer])

        hand_over(layer).start()
    for k in range(NZ // NC):
        layer = NC * k + 1 - c
        arrived(lhs.at[layer], l_recv.at[layer])

    depth = NZ * chunk
    lcols = lhs[...].reshape(depth, LANES)
    in_act = lax.broadcasted_iota(jnp.int32, (depth, LANES), 0) % chunk < SEQS * NB
    act_only = jnp.where(in_act, 1.0, 0.0).astype(BF16)
    grad_only = jnp.where(in_act, 0.0, 1.0).astype(BF16)
    both = jnp.concatenate([lcols * act_only, lcols * grad_only], axis=1).T

    for k in (0, 1, 3, 2):
        who = (x + k) % NX
        if k:
            arrived(rhs.at[who], x_recv.at[who])
        product = lax.dot_general(
            both, rhs[who].reshape(depth, LANES), (((1,), (0,)), ((), ())), preferred_element_type=F32
        )
        product = (product / total_seqs).astype(BF16)
        for d in range(NB):
            for kind in range(2):
                tiles[k, d, kind * rows : (kind + 1) * rows] = product[
                    kind * LANES + d * rows : kind * LANES + (d + 1) * rows
                ]
        for step in (4, 5, 2, 3, 6, 7, 1):
            d = (g_me + step) % NB
            pltpu.make_async_remote_copy(
                src_ref=tiles.at[k, d], dst_ref=landed.at[who, mine],
                send_sem=o_send.at[k], recv_sem=o_recv.at[who],
                device_id=at(x, d // NC, z, d % NC), device_id_type=MESH,
            ).start()
        landed[who, mine] = tiles[k, g_me]

    arrived(got.at[pl.ds(0, NX * NB - 1)], s1_send)
    arrived(rhs.at[0, pl.ds(0, NZ - 1)], z_send)
    arrived(rhs.at[pl.ds(0, NX - 1)], x_send)

    alone = (mine == z) & (z % NC == c)

    @pl.when(alone)
    def _():
        arrived(lhs.at[pl.ds(0, NY - 1)], l_send)

    @pl.when(jnp.logical_not(alone))
    def _():
        arrived(lhs.at[pl.ds(0, NY)], l_send)

    arrived(lhs.at[pl.ds(0, NZ // NC)], d_send)
    for k in range(NX):
        arrived(landed.at[k, pl.ds(0, NB - 1)], o_send.at[k])
    for q in range(NX):
        arrived(landed.at[q, pl.ds(0, NB - 1)], o_recv.at[q])
    for q in range(NX):
        for zb in range(NB):
            cols = pl.ds((q * NB + zb) * LANES, LANES)
            for kind in range(2):
                out_ref[kind, :, cols] = landed[q, zb, kind * rows : (kind + 1) * rows]


def local(activations, out_grads, lengths):
    tokens, width = activations.shape[1:]
    rows = width // (NX * NY * NZ * NC)
    steps = 2 * NX
    wide = width // steps
    chunk = 2 * SEQS * NB
    dma = pltpu.SemaphoreType.DMA
    out = pl.pallas_call(
        kernel,
        out_shape=pltpu.VMEM((2, rows, width), BF16),
        in_specs=[
            pl.BlockSpec(memory_space=pl.ANY),
            pl.BlockSpec(memory_space=pl.ANY),
            pl.BlockSpec(memory_space=pltpu.SMEM),
        ],
        out_specs=pl.BlockSpec(memory_space=pltpu.VMEM),
        scratch_shapes=[
            pltpu.VMEM((steps, tokens, wide), BF16),
            pltpu.VMEM((steps, tokens, wide), BF16),
            pltpu.VMEM((NX * NB, 8, LANES), F32),
            pltpu.VMEM((NX * NB, 8, LANES), F32),
            pltpu.VMEM((chunk, LANES), F32),
            pltpu.VMEM((NX, NZ, chunk, LANES), BF16),
            pltpu.VMEM((NZ, chunk, LANES), BF16),
            pltpu.VMEM((NX, NB, 2 * rows, LANES), BF16),
            pltpu.VMEM((NX, NB, 2 * rows, LANES), BF16),
            dma((2, steps)),
            dma, dma,
            dma, dma((NZ,)),
            dma, dma((NX,)),
            dma, dma((NZ,)), dma,
            dma((NX,)), dma((NX,)),
        ],
        compiler_params=pltpu.CompilerParams(collective_id=0, has_side_effects=True),
    )(activations, out_grads, lengths)
    return out[0].astype(F32), out[1].astype(F32)


def solution(mesh):
    in_specs = (P("batch", "seq", None), P("batch", "seq", None), P("batch", None))
    out_specs = (P(("seq", "batch"), None), P(("seq", "batch"), None))
    return jax.shard_map(local, mesh=mesh, in_specs=in_specs, out_specs=out_specs, check_vma=False)
```

```python
import jax
import jax.numpy as jnp
from jax import lax
from jax.experimental import pallas as pl
from jax.experimental.pallas import tpu as pltpu
from jax.sharding import PartitionSpec as P

NX, NY, NZ, NC = 4, 4, 8, 2
NB = NY * NC
LANES = 128
SEQS = 3
HELD = 4
MESH = pl.DeviceIdType.MESH
F32, BF16 = jnp.float32, jnp.bfloat16


def kernel(
    act_hbm, grad_hbm, len_ref, out_ref,
    abuf, gbuf, parts, got, packed, rhs, lhs, tiles, landed,
    in_sem, s1_send, s1_recv, z_send, z_recv, x_send, x_recv, l_send, l_recv, d_send, o_send, o_recv,
):
    steps, tokens, wide = abuf.shape
    halves = steps // NX
    per_step = wide // LANES
    total_seqs = SEQS * NZ * NY * NC
    rows = LANES // NB
    chunk = 2 * SEQS * NB

    x = lax.axis_index("seq")
    b = lax.axis_index("batch")
    c = b % NC
    y = (b // NC) % NY
    z = b // (NC * NY)
    mine = y + NY * c
    g_me = y * NC + c

    def at(x_, y_, z_, c_):
        return (x_, (z_ * NY + y_) * NC + c_)

    whole = steps - steps // NX
    pieces = 2 * steps // NX
    span = per_step // 2

    def blocks(i):
        if i < whole:
            return (x + 1 + i // halves) % NX, (i % halves) * per_step, per_step
        p = i - whole
        pair = y // span if p >= halves else 1 - y // span
        return x, (p % halves) * per_step + pair * span, span

    def views(i):
        if i < whole:
            return abuf.at[i], gbuf.at[i]
        slot, half = whole + (i - whole) // 2, pl.ds((i - whole) % 2 * span * LANES, span * LANES)
        return abuf.at[slot, :, half], gbuf.at[slot, :, half]

    def loads(i):
        q, first, count = blocks(i)
        cols = pl.ds(pl.multiple_of((q * NB + first) * LANES, span * LANES), count * LANES)
        a_view, g_view = views(i)
        return (
            pltpu.make_async_copy(act_hbm.at[0, :, cols], a_view, in_sem.at[0, i]),
            pltpu.make_async_copy(grad_hbm.at[0, :, cols], g_view, in_sem.at[1, i]),
        )

    for i in range(whole + pieces):
        for copy in loads(i):
            copy.start()

    barrier = pltpu.get_barrier_semaphore()

    def greet(target):
        pl.semaphore_signal(barrier, inc=1, device_id=target, device_id_type=MESH)

    src_y, src_c = z % NY, z // NY
    src_here = jnp.logical_and(src_y == y, src_c == c)

    for k in (4, 3, 5, 2, 6, 1, 7, 0):
        layer = (z + k) % NZ

        if k:
            greet(at(x, y, layer, c))

        @pl.when((layer % NC == c) & jnp.logical_not(src_here & (layer == z)))
        def _():
            greet(at(x, src_y, layer, src_c))

    for dx in (2, 1, 3, 0):
        for dy in (2, 1, 3, 0):
            for dc in range(NC):
                if dx or dy or dc:
                    greet(at((x + dx) % NX, (y + dy) % NY, z, (c + dc) % NC))

    l0, l1, l2 = len_ref[0, 0], len_ref[0, 1], len_ref[0, 2]
    row = lax.broadcasted_iota(jnp.int32, (8, tokens), 0)
    pos = lax.broadcasted_iota(jnp.int32, (8, tokens), 1) + x * tokens

    def member(first):
        r = row - first
        start = jnp.where(r == 0, 0, jnp.where(r == 1, l0, l0 + l1))
        end = jnp.where(r == 0, l0, jnp.where(r == 1, l0 + l1, l0 + l1 + l2))
        inside = (r >= 0) & (r < SEQS) & (pos >= start) & (pos < end)
        return jnp.where(inside, 1.0, 0.0).astype(BF16)

    m_act, m_grad = member(0), member(SEQS)
    row_w = lax.broadcasted_iota(jnp.int32, (8, wide), 0)
    divisor = jnp.where(row_w == 0, l0, jnp.where(row_w == 1, l1, jnp.where(row_w == 2, l2, 1))).astype(F32)

    def s1_copy(slot_block, target, slot):
        return pltpu.make_async_remote_copy(
            src_ref=parts.at[slot_block, pl.ds(0, 2 * SEQS)], dst_ref=got.at[slot, pl.ds(0, 2 * SEQS)],
            send_sem=s1_send, recv_sem=s1_recv, device_id=target, device_id_type=MESH,
        )

    my_slot = x * NB + g_me
    home = x * NB + mine

    def sums(i):
        for copy in loads(i):
            copy.wait()
        q, first, count = blocks(i)
        a_view, g_view = views(i)
        total = jnp.dot(m_act, a_view[...], preferred_element_type=F32)
        total += jnp.dot(m_grad, g_view[...], preferred_element_type=F32)
        total = total / divisor[:, : count * LANES]
        for j in range(count):
            parts[q * NB + first + j] = total[:, j * LANES : (j + 1) * LANES]

    def sends(i):
        q, first, count = blocks(i)
        for j in range(count):
            zb = first + j

            @pl.when(q * NB + zb != home)
            def _():
                s1_copy(q * NB + zb, at(q, zb % NY, z, zb // NY), my_slot).start()

    for i in range(HELD):
        sums(i)

    pl.semaphore_wait(barrier, NX * NB - 1 + NZ - 1 + NY - jnp.where((mine == z) & (z % NC == c), 1, 0))

    for i in range(HELD):
        sends(i)

    for i in range(HELD, whole + pieces):
        sums(i)
        sends(i)

    got[my_slot] = parts[home]
    pltpu.make_async_copy(got.at[pl.ds(0, NX * NB - 1), pl.ds(0, 2 * SEQS)], got.at[pl.ds(0, NX * NB - 1), pl.ds(0, 2 * SEQS)], s1_recv).wait()

    for g in range(NB):
        summed = got[g]
        for k in range(1, NX):
            summed += got[k * NB + g]
        packed[g * SEQS : (g + 1) * SEQS] = summed[0:SEQS]
        packed[SEQS * (NB + g) : SEQS * (NB + g + 1)] = summed[SEQS : 2 * SEQS]
    own = packed[...].astype(BF16)
    rhs[x, z] = own

    @pl.when((mine == z) & (z % NC == c))
    def _():
        lhs[z] = own

    def z_copy(k):
        return pltpu.make_async_remote_copy(
            src_ref=rhs.at[x, z], dst_ref=rhs.at[x, z],
            send_sem=z_send, recv_sem=z_recv.at[z],
            device_id=at(x, y, (z + k) % NZ, c), device_id_type=MESH,
        )

    def x_copy(k, layer):
        return pltpu.make_async_remote_copy(
            src_ref=rhs.at[x, layer], dst_ref=rhs.at[x, layer],
            send_sem=x_send, recv_sem=x_recv.at[x],
            device_id=at((x + k) % NX, y, z, c), device_id_type=MESH,
        )

    def l_copy(d):
        return pltpu.make_async_remote_copy(
            src_ref=rhs.at[x, z], dst_ref=lhs.at[z],
            send_sem=l_send, recv_sem=l_recv.at[z],
            device_id=at(x, d // NC, mine, d % NC), device_id_type=MESH,
        )

    for k in (4, 3, 5, 2, 6, 1, 7):
        z_copy(k).start()
    for k in (2, 1, 3):
        x_copy(k, z).start()
    for k in (2, 1, 3, 0):
        to_y = (y + k) % NY

        @pl.when(jnp.logical_not((mine == z) & (z % NC == c) & (to_y == y)))
        def _():
            l_copy(to_y * NC + z % NC).start()

    def arrived(ref, sem):
        pltpu.make_async_copy(ref, ref, sem).wait()

    for k in (1, 7, 2, 6, 3, 5, 4):
        layer = (z + k) % NZ
        arrived(rhs.at[x, layer], z_recv.at[layer])
        for kx in (2, 1, 3):
            x_copy(kx, layer).start()

    def hand_over(layer):
        return pltpu.make_async_remote_copy(
            src_ref=lhs.at[layer], dst_ref=lhs.at[layer],
            send_sem=d_send, recv_sem=l_recv.at[layer],
            device_id=at(x, y, z, 1 - c), device_id_type=MESH,
        )

    for k in range(NZ // NC):
        layer = (z + c + z % NC + (0, 6, 2, 4)[k]) % NZ

        @pl.when(jnp.logical_not(src_here & (layer == z)))
        def _():
            arrived(lhs.at[layer], l_recv.at[layer])

        hand_over(layer).start()
    for k in range(NZ // NC):
        layer = NC * k + 1 - c
        arrived(lhs.at[layer], l_recv.at[layer])

    depth = NZ * chunk
    lcols = lhs[...].reshape(depth, LANES)
    in_act = lax.broadcasted_iota(jnp.int32, (depth, LANES), 0) % chunk < SEQS * NB
    act_only = jnp.where(in_act, 1.0, 0.0).astype(BF16)
    grad_only = jnp.where(in_act, 0.0, 1.0).astype(BF16)
    both = jnp.concatenate([lcols * act_only, lcols * grad_only], axis=1).T

    for k in (0, 1, 3, 2):
        who = (x + k) % NX
        if k:
            arrived(rhs.at[who], x_recv.at[who])
        product = lax.dot_general(
            both, rhs[who].reshape(depth, LANES), (((1,), (0,)), ((), ())), preferred_element_type=F32
        )
        product = (product / total_seqs).astype(BF16)
        for d in range(NB):
            for kind in range(2):
                tiles[k, d, kind * rows : (kind + 1) * rows] = product[
                    kind * LANES + d * rows : kind * LANES + (d + 1) * rows
                ]
        for step in (4, 5, 2, 3, 6, 7, 1):
            d = (g_me + step) % NB
            pltpu.make_async_remote_copy(
                src_ref=tiles.at[k, d], dst_ref=landed.at[who, mine],
                send_sem=o_send.at[k], recv_sem=o_recv.at[who],
                device_id=at(x, d // NC, z, d % NC), device_id_type=MESH,
            ).start()
        landed[who, mine] = tiles[k, g_me]

    arrived(got.at[pl.ds(0, NX * NB - 1), pl.ds(0, 2 * SEQS)], s1_send)
    arrived(rhs.at[0, pl.ds(0, NZ - 1)], z_send)
    arrived(rhs.at[pl.ds(0, NX - 1)], x_send)

    alone = (mine == z) & (z % NC == c)

    @pl.when(alone)
    def _():
        arrived(lhs.at[pl.ds(0, NY - 1)], l_send)

    @pl.when(jnp.logical_not(alone))
    def _():
        arrived(lhs.at[pl.ds(0, NY)], l_send)

    arrived(lhs.at[pl.ds(0, NZ // NC)], d_send)
    for k in range(NX):
        arrived(landed.at[k, pl.ds(0, NB - 1)], o_send.at[k])
    for q in range(NX):
        arrived(landed.at[q, pl.ds(0, NB - 1)], o_recv.at[q])
    for q in range(NX):
        for zb in range(NB):
            cols = pl.ds((q * NB + zb) * LANES, LANES)
            for kind in range(2):
                out_ref[kind, :, cols] = landed[q, zb, kind * rows : (kind + 1) * rows]


def local(activations, out_grads, lengths):
    tokens, width = activations.shape[1:]
    rows = width // (NX * NY * NZ * NC)
    steps = 2 * NX
    wide = width // steps
    chunk = 2 * SEQS * NB
    dma = pltpu.SemaphoreType.DMA
    out = pl.pallas_call(
        kernel,
        out_shape=pltpu.VMEM((2, rows, width), BF16),
        in_specs=[
            pl.BlockSpec(memory_space=pl.ANY),
            pl.BlockSpec(memory_space=pl.ANY),
            pl.BlockSpec(memory_space=pltpu.SMEM),
        ],
        out_specs=pl.BlockSpec(memory_space=pltpu.VMEM),
        scratch_shapes=[
            pltpu.VMEM((steps, tokens, wide), BF16),
            pltpu.VMEM((steps, tokens, wide), BF16),
            pltpu.VMEM((NX * NB, 8, LANES), F32),
            pltpu.VMEM((NX * NB, 8, LANES), F32),
            pltpu.VMEM((chunk, LANES), F32),
            pltpu.VMEM((NX, NZ, chunk, LANES), BF16),
            pltpu.VMEM((NZ, chunk, LANES), BF16),
            pltpu.VMEM((NX, NB, 2 * rows, LANES), BF16),
            pltpu.VMEM((NX, NB, 2 * rows, LANES), BF16),
            dma((2, steps + steps // NX)),
            dma, dma,
            dma, dma((NZ,)),
            dma, dma((NX,)),
            dma, dma((NZ,)), dma,
            dma((NX,)), dma((NX,)),
        ],
        compiler_params=pltpu.CompilerParams(collective_id=0, has_side_effects=True),
    )(activations, out_grads, lengths)
    return out[0].astype(F32), out[1].astype(F32)


def solution(mesh):
    in_specs = (P("batch", "seq", None), P("batch", "seq", None), P("batch", None))
    out_specs = (P(("seq", "batch"), None), P(("seq", "batch"), None))
    return jax.shard_map(local, mesh=mesh, in_specs=in_specs, out_specs=out_specs, check_vma=False)
```

```python
import jax
import jax.numpy as jnp
from jax import lax
from jax.experimental import pallas as pl
from jax.experimental.pallas import tpu as pltpu
from jax.sharding import PartitionSpec as P

NX, NY, NZ, NC = 4, 4, 8, 2
NB = NY * NC
LANES = 128
SEQS = 3
HELD = 4
MESH = pl.DeviceIdType.MESH
F32, BF16 = jnp.float32, jnp.bfloat16


def kernel(
    act_hbm, grad_hbm, len_ref, out_ref,
    abuf, gbuf, parts, got, packed, rhs, lhs, tiles, landed,
    in_sem, s1_send, s1_recv, z_send, z_recv, x_send, x_recv, l_send, l_recv, d_send, o_send, o_recv,
):
    steps, tokens, wide = abuf.shape
    halves = steps // NX
    per_step = wide // LANES
    total_seqs = SEQS * NZ * NY * NC
    rows = LANES // NB
    chunk = 2 * SEQS * NB

    x = lax.axis_index("seq")
    b = lax.axis_index("batch")
    c = b % NC
    y = (b // NC) % NY
    z = b // (NC * NY)
    mine = y + NY * c
    g_me = y * NC + c

    def at(x_, y_, z_, c_):
        return (x_, (z_ * NY + y_) * NC + c_)

    whole = steps - steps // NX
    pieces = 2 * steps // NX
    span = per_step // 2

    def blocks(i):
        if i < whole:
            return (x + 1 + i // halves) % NX, (i % halves) * per_step, per_step
        p = i - whole
        pair = y // span if p >= halves else 1 - y // span
        return x, (p % halves) * per_step + pair * span, span

    def views(i):
        if i < whole:
            return abuf.at[i], gbuf.at[i]
        slot, half = whole + (i - whole) // 2, pl.ds((i - whole) % 2 * span * LANES, span * LANES)
        return abuf.at[slot, :, half], gbuf.at[slot, :, half]

    def loads(i):
        q, first, count = blocks(i)
        cols = pl.ds(pl.multiple_of((q * NB + first) * LANES, span * LANES), count * LANES)
        a_view, g_view = views(i)
        return (
            pltpu.make_async_copy(act_hbm.at[0, :, cols], a_view, in_sem.at[0, i]),
            pltpu.make_async_copy(grad_hbm.at[0, :, cols], g_view, in_sem.at[1, i]),
        )

    for i in range(whole + pieces):
        for copy in loads(i):
            copy.start()

    barrier = pltpu.get_barrier_semaphore()

    def greet(target):
        pl.semaphore_signal(barrier, inc=1, device_id=target, device_id_type=MESH)

    src_y, src_c = z % NY, z // NY
    src_here = jnp.logical_and(src_y == y, src_c == c)

    for k in (4, 3, 5, 2, 6, 1, 7, 0):
        layer = (z + k) % NZ

        if k:
            greet(at(x, y, layer, c))

        @pl.when((layer % NC == c) & jnp.logical_not(src_here & (layer == z)))
        def _():
            greet(at(x, src_y, layer, src_c))

    for dx in (2, 1, 3, 0):
        for dy in (2, 1, 3, 0):
            for dc in range(NC):
                if dx or dy or dc:
                    greet(at((x + dx) % NX, (y + dy) % NY, z, (c + dc) % NC))

    l0, l1, l2 = len_ref[0, 0], len_ref[0, 1], len_ref[0, 2]
    row = lax.broadcasted_iota(jnp.int32, (8, tokens), 0)
    pos = lax.broadcasted_iota(jnp.int32, (8, tokens), 1) + x * tokens

    def member(first):
        r = row - first
        start = jnp.where(r == 0, 0, jnp.where(r == 1, l0, l0 + l1))
        end = jnp.where(r == 0, l0, jnp.where(r == 1, l0 + l1, l0 + l1 + l2))
        inside = (r >= 0) & (r < SEQS) & (pos >= start) & (pos < end)
        return jnp.where(inside, 1.0, 0.0).astype(BF16)

    m_act, m_grad = member(0), member(SEQS)
    row_w = lax.broadcasted_iota(jnp.int32, (8, wide), 0)
    divisor = jnp.where(row_w == 0, l0, jnp.where(row_w == 1, l1, jnp.where(row_w == 2, l2, 1))).astype(F32)

    def s1_copy(slot_block, target, slot):
        return pltpu.make_async_remote_copy(
            src_ref=parts.at[slot_block, pl.ds(0, 2 * SEQS)], dst_ref=got.at[slot, pl.ds(0, 2 * SEQS)],
            send_sem=s1_send, recv_sem=s1_recv, device_id=target, device_id_type=MESH,
        )

    my_slot = x * NB + g_me
    home = x * NB + mine

    def sums(i):
        for copy in loads(i):
            copy.wait()
        q, first, count = blocks(i)
        a_view, g_view = views(i)
        total = jnp.dot(m_act, a_view[...], preferred_element_type=F32)
        total += jnp.dot(m_grad, g_view[...], preferred_element_type=F32)
        total = total / divisor[:, : count * LANES]
        for j in range(count):
            parts[q * NB + first + j] = total[:, j * LANES : (j + 1) * LANES]

    def sends(i):
        q, first, count = blocks(i)
        for j in range(count):
            zb = first + j

            @pl.when(q * NB + zb != home)
            def _():
                s1_copy(q * NB + zb, at(q, zb % NY, z, zb // NY), my_slot).start()

    for i in range(HELD):
        sums(i)

    pl.semaphore_wait(barrier, NX * NB - 1 + NZ - 1 + NY - jnp.where((mine == z) & (z % NC == c), 1, 0))

    for i in range(HELD):
        sends(i)

    for i in range(HELD, whole + pieces):
        sums(i)
        sends(i)

    got[my_slot] = parts[home]
    pltpu.make_async_copy(got.at[pl.ds(0, NX * NB - 1), pl.ds(0, 2 * SEQS)], got.at[pl.ds(0, NX * NB - 1), pl.ds(0, 2 * SEQS)], s1_recv).wait()

    for g in range(NB):
        summed = got[g]
        for k in range(1, NX):
            summed += got[k * NB + g]
        packed[g * SEQS : (g + 1) * SEQS] = summed[0:SEQS]
        packed[SEQS * (NB + g) : SEQS * (NB + g + 1)] = summed[SEQS : 2 * SEQS]
    own = packed[...].astype(BF16)
    rhs[x, z] = own

    @pl.when((mine == z) & (z % NC == c))
    def _():
        lhs[z] = own

    def z_copy(k):
        return pltpu.make_async_remote_copy(
            src_ref=rhs.at[x, z], dst_ref=rhs.at[x, z],
            send_sem=z_send, recv_sem=z_recv.at[z],
            device_id=at(x, y, (z + k) % NZ, c), device_id_type=MESH,
        )

    def x_copy(k, layer):
        return pltpu.make_async_remote_copy(
            src_ref=rhs.at[x, layer], dst_ref=rhs.at[x, layer],
            send_sem=x_send, recv_sem=x_recv.at[x],
            device_id=at((x + k) % NX, y, z, c), device_id_type=MESH,
        )

    def l_copy(d):
        return pltpu.make_async_remote_copy(
            src_ref=rhs.at[x, z], dst_ref=lhs.at[z],
            send_sem=l_send, recv_sem=l_recv.at[z],
            device_id=at(x, d // NC, mine, d % NC), device_id_type=MESH,
        )

    for k in (4, 3, 5, 2, 6, 1, 7):
        z_copy(k).start()
    for k in (2, 1, 3):
        x_copy(k, z).start()
    for k in (2, 1, 3, 0):
        to_y = (y + k) % NY

        @pl.when(jnp.logical_not((mine == z) & (z % NC == c) & (to_y == y)))
        def _():
            l_copy(to_y * NC + z % NC).start()

    def arrived(ref, sem):
        pltpu.make_async_copy(ref, ref, sem).wait()

    for k in (1, 7, 2, 6, 3, 5, 4):
        layer = (z + k) % NZ
        arrived(rhs.at[x, layer], z_recv.at[layer])
        for kx in (2, 1, 3):
            x_copy(kx, layer).start()

    def hand_over(layer):
        return pltpu.make_async_remote_copy(
            src_ref=lhs.at[layer], dst_ref=lhs.at[layer],
            send_sem=d_send, recv_sem=l_recv.at[layer],
            device_id=at(x, y, z, 1 - c), device_id_type=MESH,
        )

    for k in range(NZ // NC):
        layer = (z + c + z % NC + (0, 6, 2, 4)[k]) % NZ

        @pl.when(jnp.logical_not(src_here & (layer == z)))
        def _():
            arrived(lhs.at[layer], l_recv.at[layer])

        hand_over(layer).start()
    for k in range(NZ // NC):
        layer = NC * k + 1 - c
        arrived(lhs.at[layer], l_recv.at[layer])

    depth = NZ * chunk
    lcols = lhs[...].reshape(depth, LANES)
    in_act = lax.broadcasted_iota(jnp.int32, (depth, LANES), 0) % chunk < SEQS * NB
    act_only = jnp.where(in_act, 1.0, 0.0).astype(BF16)
    grad_only = jnp.where(in_act, 0.0, 1.0).astype(BF16)
    both = jnp.concatenate([lcols * act_only, lcols * grad_only], axis=1).T

    for k in (0, 1, 3, 2):
        who = (x + k) % NX
        if k:
            arrived(rhs.at[who], x_recv.at[who])
        product = lax.dot_general(
            both, rhs[who].reshape(depth, LANES), (((1,), (0,)), ((), ())), preferred_element_type=F32
        )
        product = (product / total_seqs).astype(BF16)
        for d in range(NB):
            for kind in range(2):
                tiles[k, d, kind * rows : (kind + 1) * rows] = product[
                    kind * LANES + d * rows : kind * LANES + (d + 1) * rows
                ]
        for step in (4, 5, 2, 3, 6, 7, 1):
            d = (g_me + step) % NB
            pltpu.make_async_remote_copy(
                src_ref=tiles.at[k, d], dst_ref=landed.at[who, mine],
                send_sem=o_send.at[k], recv_sem=o_recv.at[who],
                device_id=at(x, d // NC, z, d % NC), device_id_type=MESH,
            ).start()
        landed[who, mine] = tiles[k, g_me]

    for k in (0, 1, 3, 2):
        who = (x + k) % NX
        arrived(landed.at[who, pl.ds(0, NB - 1)], o_recv.at[who])
        for zb in range(NB):
            cols = pl.ds(pl.multiple_of((who * NB + zb) * LANES, LANES), LANES)
            for kind in range(2):
                out_ref[kind, :, cols] = landed[who, zb, kind * rows : (kind + 1) * rows]

    arrived(got.at[pl.ds(0, NX * NB - 1), pl.ds(0, 2 * SEQS)], s1_send)
    arrived(rhs.at[0, pl.ds(0, NZ - 1)], z_send)
    arrived(rhs.at[pl.ds(0, NX - 1)], x_send)

    alone = (mine == z) & (z % NC == c)

    @pl.when(alone)
    def _():
        arrived(lhs.at[pl.ds(0, NY - 1)], l_send)

    @pl.when(jnp.logical_not(alone))
    def _():
        arrived(lhs.at[pl.ds(0, NY)], l_send)

    arrived(lhs.at[pl.ds(0, NZ // NC)], d_send)
    for k in range(NX):
        arrived(landed.at[k, pl.ds(0, NB - 1)], o_send.at[k])


def local(activations, out_grads, lengths):
    tokens, width = activations.shape[1:]
    rows = width // (NX * NY * NZ * NC)
    steps = 2 * NX
    wide = width // steps
    chunk = 2 * SEQS * NB
    dma = pltpu.SemaphoreType.DMA
    out = pl.pallas_call(
        kernel,
        out_shape=pltpu.VMEM((2, rows, width), BF16),
        in_specs=[
            pl.BlockSpec(memory_space=pl.ANY),
            pl.BlockSpec(memory_space=pl.ANY),
            pl.BlockSpec(memory_space=pltpu.SMEM),
        ],
        out_specs=pl.BlockSpec(memory_space=pltpu.VMEM),
        scratch_shapes=[
            pltpu.VMEM((steps, tokens, wide), BF16),
            pltpu.VMEM((steps, tokens, wide), BF16),
            pltpu.VMEM((NX * NB, 8, LANES), F32),
            pltpu.VMEM((NX * NB, 8, LANES), F32),
            pltpu.VMEM((chunk, LANES), F32),
            pltpu.VMEM((NX, NZ, chunk, LANES), BF16),
            pltpu.VMEM((NZ, chunk, LANES), BF16),
            pltpu.VMEM((NX, NB, 2 * rows, LANES), BF16),
            pltpu.VMEM((NX, NB, 2 * rows, LANES), BF16),
            dma((2, steps + steps // NX)),
            dma, dma,
            dma, dma((NZ,)),
            dma, dma((NX,)),
            dma, dma((NZ,)), dma,
            dma((NX,)), dma((NX,)),
        ],
        compiler_params=pltpu.CompilerParams(collective_id=0, has_side_effects=True),
    )(activations, out_grads, lengths)
    return out[0].astype(F32), out[1].astype(F32)


def solution(mesh):
    in_specs = (P("batch", "seq", None), P("batch", "seq", None), P("batch", None))
    out_specs = (P(("seq", "batch"), None), P(("seq", "batch"), None))
    return jax.shard_map(local, mesh=mesh, in_specs=in_specs, out_specs=out_specs, check_vma=False)
```
